32 devices in a mesh: fsdp: 8 (over z, core), tp: 4 (over y, x).
Axes of the slice: x: 2, y: 2, z: 4, core: 2. Of those that a mesh axis runs over, the one named last changes fastest.
Arguments:
- hidden_in: bfloat16 [512, 4096], P('fsdp'), may hold values from -3 to 3
- queries: bfloat16 [2, 512, 8192], P(None, ('fsdp', 'tp')), may hold values from -170 to 170
- key_cache: bfloat16 [512, 256, 512], P(('fsdp', 'tp')), may hold values from -6 to 6
- value_cache: bfloat16 [512, 256, 512], P(('fsdp', 'tp')), may hold values from -6 to 6
- new_keys: bfloat16 [2, 512, 512], P(None, ('fsdp', 'tp')), may hold values from -6 to 6
- new_values: bfloat16 [2, 512, 512], P(None, ('fsdp', 'tp')), may hold values from -6 to 6
- lengths: int32 [512], P(('fsdp', 'tp')), may hold values from 2 to 256
- routes: int32 [2, 512, 8], P(None, 'fsdp'), may hold values from 0 to 127, all different within a row; in each aligned block of 64 rows (0 to 63, 64 to 127, ..., all dimensions but the last counted through in order) at most 8 rows name the same one
- route_weights: float32 [2, 512, 8], P(None, 'fsdp'), may hold values from 0.05 to 1
- norm_gain: float32 [4096], replicated, may hold values from 0.1 to 1.9
- gate_master: float32 [8, 1536, 4096], P(None, ('fsdp', 'tp')), may hold values from -0.09375 to 0.09375
- up_master: float32 [8, 1536, 4096], P(None, ('fsdp', 'tp')), may hold values from -0.09375 to 0.09375
- down_master: float32 [8, 1536, 4096], P(None, ('fsdp', 'tp')), may hold values from -0.3125 to 0.3125
- out_proj: bfloat16 [8192, 4096], P('tp'), may hold values from -0.0625 to 0.0625
Outputs:
- hidden_out: bfloat16 [512, 4096], P('fsdp', 'tp')
- scale_log2: float32 [3, 8, 12, 32], replicated
The draws below stay inside these ranges and needn't reach their ends.
Inputs may be any that keep to these rules, and one draw needn't show every extreme that they name: `routes`: within one step and one index of fsdp (aligned blocks of 64 rows), no expert is named by more than 8 rows.
All inputs are finite; a program needn't handle non-finite values.
Results may differ from the reference program's by a relative error of at most 0.0095.
Values may be sent and summed in bfloat16 or wider, within the bound.
No kernel may reach another device: no remote copies, remote signals or barrier semaphores. Data moves between devices by JAX's collectives and lax.ppermute only.
A program may use at most 384 MiB of HBM per device.

```python
import math
import jax
import jax.numpy as jnp
import numpy as np
from jax import lax

D = 4096
FF = 1536
EXPERTS = 128
TOPK = 8
QH = 64
KVH = 4
HD = 128
BLOCK = 128
WIN = 8
STEPS = 2
ROWS = 64
CACHE = 256
TOKENS = 512
CAP = 8
N_FSDP = 8


def drawn_pair(key):
    cache_keys = jnp.clip(jax.random.normal(jax.random.fold_in(key, 101), (TOKENS, CACHE, KVH * HD), jnp.float32), -6.0, 6.0)
    query_draw = jnp.clip(jax.random.normal(jax.random.fold_in(key, 102), (STEPS, TOKENS, QH * HD), jnp.float32), -6.0, 6.0)
    return (query_draw, cache_keys)


def draw_queries(key, part):
    query_draw, cache_keys = drawn_pair(key)
    return query_draw.astype(jnp.bfloat16)


def draw_key_cache(key, part):
    query_draw, cache_keys = drawn_pair(key)
    return cache_keys.astype(jnp.bfloat16)


def place_ends(entries, rng, low, high):
    extent = entries.shape
    spot = [jax.random.randint(jax.random.fold_in(rng, axis), (), 0, extent[axis]) for axis in range(len(extent))]
    entries = entries.at[tuple(spot)].set(low)
    longest = extent.index(max(extent))
    spot[longest] = (spot[longest] + 1) % extent[longest]
    return entries.at[tuple(spot)].set(high)


def level_of(rng, shape, split, smallest, high):
    loudness, own = 1.0, jax.random.fold_in(rng, 6)
    for dim, parts in split:
        draws = jnp.exp(jax.random.uniform(jax.random.fold_in(own, dim), (parts,), jnp.float32, smallest / len(split), high / len(split)))
        loudness = loudness * jnp.repeat(draws, shape[dim] // parts).reshape([-1 if axis == dim else 1 for axis in range(len(shape))])
    return loudness


def routed_block(own_key, own, number, rows, number_of, top, bound, slope):
    ranking = jax.random.permutation(own_key, number_of)
    heavy_load, ordinary = shares(number_of, rows * top, bound, slope, True), shares(number_of, rows * top, bound, slope, False)
    places = jnp.arange(number_of)

    def named(tallies, offset_by):
        used = int((tallies > 0).sum())
        fixed = max(1, used // 4)
        moved = fixed + (places - fixed + offset_by * (used - fixed)) % max(1, number_of - fixed)
        return jnp.zeros((number_of,), jnp.int32).at[ranking[jnp.where(places < fixed, places, moved)]].set(jnp.asarray(tallies, jnp.int32))

    tallies = jnp.where(number % 4 == 0, named(heavy_load, number // 4), named(ordinary, number - number // 4 - 1))
    mixed = jax.random.permutation(jax.random.fold_in(own, 3), number_of)
    source_of, sink = mixed[0:number_of // 2 * 2:2], mixed[1:number_of // 2 * 2:2]
    slack = jnp.minimum(tallies[source_of] - 1, bound - tallies[sink]) // 2
    slack = jnp.where((source_of == ranking[0]) | (sink == ranking[0]) | (tallies[sink] == 0), 0, jnp.maximum(slack, 0))
    moved = jax.random.randint(jax.random.fold_in(own, 4), (number_of // 2,), 0, 1 << 20) % (slack + 1)
    tallies = tallies.at[source_of].add(-moved).at[sink].add(moved)
    labels = jnp.searchsorted(jnp.cumsum(tallies), jnp.arange(rows * top), side="right").astype(jnp.int32)
    grid = labels.reshape(top, rows).T
    grid = grid[jax.random.permutation(jax.random.fold_in(own, 1), rows)]
    offset_by = jax.random.randint(jax.random.fold_in(own, 2), (rows, 1), 0, top)
    return jnp.take_along_axis(grid, (jnp.arange(top)[None, :] + offset_by) % top, axis=1)


def shares(number_of, total, bound, skew, full):
    weights = [(1 << 20) // math.isqrt(rank ** skew) + 1 for rank in range(1, number_of + 1)]
    largest = bound if full else min(bound, max(-(-total // number_of), total * weights[0] // sum(weights)))
    least = 1 if total - largest >= number_of - 1 else 0
    given, rest = [largest] + [least] * (number_of - 1), total - largest - least * (number_of - 1)
    while rest > 0:
        movable = [i for i in range(1, number_of) if given[i] < largest] or [i for i in range(1, number_of) if given[i] < bound]
        whole, left = sum([weights[i] for i in movable]), rest
        for i in movable:
            addition = min(bound - given[i], max(1, left * weights[i] // whole), rest)
            given[i] = given[i] + addition
            rest = rest - addition
    return np.array(given)


def scatter_about(stream_key, dims, spread, bound, cuts=(), kind=jnp.bfloat16):
    gain = level_of(stream_key, dims, cuts, -0.22, 0.18) if cuts else 1.0
    entries = jax.random.normal(stream_key, dims, jnp.float32) * spread * gain
    return jnp.minimum(jnp.maximum(entries, -bound), bound).astype(kind)


def setup_inputs(seed: int = 0) -> dict:
    streams_of = jax.random.split(jax.random.key(seed), 15)
    hidden_in = scatter_about(streams_of[0], (TOKENS, D), 0.5, 3.0, ((0, 8),))
    queries = draw_queries(jax.random.fold_in(streams_of[14], 71), 0)
    key_cache = draw_key_cache(jax.random.fold_in(streams_of[14], 71), 0)
    value_cache = scatter_about(streams_of[3], (TOKENS, CACHE, KVH * HD), 1.0, 6.0, ((0, 32),))
    new_keys = scatter_about(streams_of[4], (STEPS, TOKENS, KVH * HD), 1.0, 6.0, ((1, 32),))
    new_values = scatter_about(streams_of[5], (STEPS, TOKENS, KVH * HD), 1.0, 6.0, ((1, 32),))
    lengths = place_ends(jax.random.randint(streams_of[6], (TOKENS,), 2, CACHE + 1), jax.random.fold_in(streams_of[6], 1), 2, CACHE).astype(jnp.int32)
    routes_keys = jax.random.split(jax.random.fold_in(streams_of[7], 1), STEPS * TOKENS // ROWS)
    routes_turns = jax.random.permutation(jax.random.fold_in(streams_of[7], 3), STEPS * TOKENS // ROWS)
    routes = jax.vmap(lambda own, number: routed_block(jax.random.fold_in(streams_of[7], 2), own, number, ROWS, EXPERTS, TOPK, CAP, 2))(routes_keys, routes_turns).reshape((STEPS, TOKENS, TOPK))
    route_weights = jnp.clip(jnp.exp(math.log(1.0) - 2.9957323 * jax.random.uniform(streams_of[8], (STEPS, TOKENS, TOPK), jnp.float32) ** level_of(streams_of[8], (STEPS, TOKENS, TOPK), ((1, 8),), -0.2, 0.2)), 0.05, 1.0)
    norm_gain = jnp.clip(1.0 + 0.18 * jax.random.normal(streams_of[9], (D,), jnp.float32), 0.1, 1.9)
    gate_master = scatter_about(streams_of[10], (WIN, FF, D), D ** -0.5, 0.09375, ((1, 32),), jnp.float32)
    up_master = scatter_about(streams_of[11], (WIN, FF, D), D ** -0.5, 0.09375, ((1, 32),), jnp.float32)
    down_master = scatter_about(streams_of[12], (WIN, FF, D), (FF // 4) ** -0.5, 0.3125, ((1, 32),), jnp.float32)
    out_proj = scatter_about(streams_of[13], (QH * HD, D), (QH * HD) ** -0.5, 0.0625, ((0, 4),))
    return dict(hidden_in=hidden_in, queries=queries, key_cache=key_cache, value_cache=value_cache, new_keys=new_keys, new_values=new_values, lengths=lengths, routes=routes, route_weights=route_weights, norm_gain=norm_gain, gate_master=gate_master, up_master=up_master, down_master=down_master, out_proj=out_proj)


neg_fill = -1e+30
epsilon = 1e-06
fp_limit = 448.0
grid_floor = 2.0 ** (-10)
least_exponent = -6.0

def grid_round(values):
    magnitude = jnp.abs(values)
    exponent = jnp.maximum(jnp.floor(jnp.log2(jnp.maximum(magnitude, grid_floor))), least_exponent)
    spacing = jnp.exp2(exponent - 3.0)
    return jnp.sign(values) * jnp.floor(magnitude / spacing + 0.5) * spacing

def quantize(master):
    tiles = master.reshape(WIN, FF // BLOCK, BLOCK, D // BLOCK, BLOCK)
    block_max = lax.optimization_barrier(jnp.max(jnp.abs(tiles), axis=(2, 4)))
    scales = (block_max + epsilon) / fp_limit
    quantized = grid_round(tiles / scales[:, :, None, :, None]).astype(jnp.bfloat16)
    restored = (quantized.astype(jnp.float32) * scales[:, :, None, :, None]).astype(jnp.bfloat16)
    return (restored.reshape(WIN, FF, D), jnp.log2(scales))

def rounded(values):
    return lax.optimization_barrier(values.astype(jnp.bfloat16)).astype(jnp.float32)

def attention_rows(queries_now, cache_keys, cache_values, fresh_keys, fresh_values, lengths):
    row_count = queries_now.shape[0]
    positions = cache_keys.shape[1]
    group = QH // KVH
    score_scale = HD ** (-0.5)
    query_heads = queries_now.astype(jnp.float32).reshape(row_count, KVH, group, HD)
    key_heads = cache_keys.astype(jnp.float32).reshape(row_count, positions, KVH, HD)
    value_heads = cache_values.astype(jnp.float32).reshape(row_count, positions, KVH, HD)
    fresh_count = fresh_keys.shape[1]
    fresh_key_heads = fresh_keys.astype(jnp.float32).reshape(row_count, fresh_count, KVH, HD)
    fresh_value_heads = fresh_values.astype(jnp.float32).reshape(row_count, fresh_count, KVH, HD)
    cached_scores = jnp.einsum('rkgd,rpkd->rkgp', query_heads, key_heads) * score_scale
    fresh_scores = jnp.einsum('rkgd,rskd->rkgs', query_heads, fresh_key_heads) * score_scale
    alive_mask = (jnp.arange(positions, dtype=jnp.int32)[None, :] < lengths[:, None])[:, None, None, :]
    peak_score = jnp.maximum(lax.optimization_barrier(jnp.max(jnp.where(alive_mask, cached_scores, neg_fill), axis=-1)), lax.optimization_barrier(jnp.max(fresh_scores, axis=-1)))
    cached_weights = jnp.where(alive_mask, jnp.exp(cached_scores - peak_score[..., None]), 0.0)
    fresh_weights = jnp.exp(fresh_scores - peak_score[..., None])
    weight_sum = lax.optimization_barrier(jnp.sum(cached_weights, axis=-1)) + lax.optimization_barrier(jnp.sum(fresh_weights, axis=-1))
    cached_probs = rounded(cached_weights / weight_sum[..., None])
    fresh_probs = rounded(fresh_weights / weight_sum[..., None])
    output = jnp.einsum('rkgp,rpkd->rkgd', cached_probs, value_heads) + jnp.einsum('rkgs,rskd->rkgd', fresh_probs, fresh_value_heads)
    return output.astype(jnp.bfloat16).reshape(row_count, QH * HD)

def rms_norm(mixed, norm_gain):
    values = mixed.astype(jnp.float32)
    inverse = lax.rsqrt(lax.optimization_barrier(jnp.mean(values * values, axis=-1, keepdims=True)) + epsilon)
    return (values * inverse * norm_gain[None, :]).astype(jnp.bfloat16)

def routing_tables(routes, route_weights, capacity):
    weight_sum = lax.optimization_barrier(jnp.sum(route_weights, axis=1))
    experts = jnp.arange(WIN, dtype=jnp.int32)
    matches = routes[None, :, :] == experts[:, None, None]
    chosen = jnp.any(matches, axis=2)
    gate_share = lax.optimization_barrier(jnp.sum(jnp.where(matches, route_weights[None, :, :], 0.0), axis=2)) / weight_sum[None, :]
    slot_index = jnp.cumsum(chosen.astype(jnp.int32), axis=1) - 1
    places = jnp.arange(capacity, dtype=jnp.int32)
    picked = (slot_index[:, None, :] == places[None, :, None]) & chosen[:, None, :]
    return (picked.astype(jnp.float32), picked.astype(jnp.float32) * gate_share[:, None, :])

def expert_rows(selected, gate_rows, up_rows, down_rows):
    gate_act = jnp.einsum('ecd,ehd->ech', selected.astype(jnp.float32), gate_rows.astype(jnp.float32))
    up_act = jnp.einsum('ecd,ehd->ech', selected.astype(jnp.float32), up_rows.astype(jnp.float32))
    product = (jax.nn.silu(gate_act) * up_act).astype(jnp.bfloat16)
    return jnp.einsum('ech,ehd->ecd', product.astype(jnp.float32), down_rows.astype(jnp.float32))

def reference(hidden_in, queries, key_cache, value_cache, new_keys, new_values, lengths, routes, route_weights, norm_gain, gate_master, up_master, down_master, out_proj):
    gate_rows, gate_log = quantize(gate_master)
    up_rows, up_log = quantize(up_master)
    down_rows, down_log = quantize(down_master)
    scale_log2 = jnp.stack([gate_log, up_log, down_log])
    block_count = TOKENS // ROWS
    width = KVH * HD
    current = hidden_in
    for step_index in range(STEPS):
        fresh_count = step_index + 1
        fresh_keys = jnp.transpose(new_keys[:fresh_count], (1, 0, 2)).reshape(block_count, ROWS, fresh_count, width)
        fresh_values = jnp.transpose(new_values[:fresh_count], (1, 0, 2)).reshape(block_count, ROWS, fresh_count, width)
        blocked = (queries[step_index].reshape(block_count, ROWS, QH * HD), key_cache.reshape(block_count, ROWS, CACHE, width), value_cache.reshape(block_count, ROWS, CACHE, width), fresh_keys, fresh_values, lengths.reshape(block_count, ROWS))
        heads = lax.map(lambda items: attention_rows(*items), blocked).reshape(TOKENS, QH * HD)
        projected = jnp.dot(heads, out_proj, preferred_element_type=jnp.float32)
        mixed = (current.astype(jnp.float32) + projected).astype(jnp.bfloat16)
        normed = rms_norm(mixed, norm_gain)
        picked, weighted = routing_tables(routes[step_index], route_weights[step_index], CAP * N_FSDP)
        selected = jnp.einsum('ecr,rd->ecd', picked, normed.astype(jnp.float32)).astype(jnp.bfloat16)
        outputs = expert_rows(selected, gate_rows, up_rows, down_rows)
        moe = jnp.einsum('ecr,ecd->rd', weighted, outputs, precision=lax.Precision.HIGHEST)
        current = (mixed.astype(jnp.float32) + moe).astype(jnp.bfloat16)
    return (current, scale_log2)
```

```python
import functools
import math

import jax
import jax.numpy as jnp
from jax import lax
from jax.experimental import pallas as pl
from jax.experimental.pallas import tpu as pltpu
from jax.sharding import Mesh, PartitionSpec as P


QH = 64
KVH = 4
HD = 128
BLOCK = 128
WIN = 8

neg_fill = -1e30
epsilon = 1e-06
fp_limit = 448.0
f32 = jnp.float32
bf16 = jnp.bfloat16


def shift(value, axis, size, amount):
    return lax.ppermute(value, axis, [(i, (i + amount) % size) for i in range(size)])


def shifts(value, axis, size):
    return [value] + [shift(value, axis, size, s) for s in range(1, size)]


def attention_rows(queries_now, cache_keys, cache_values, fresh_keys, fresh_values, lengths):
    row_count = queries_now.shape[0]
    positions = cache_keys.shape[1]
    group = QH // KVH
    score_scale = HD ** (-0.5)
    fresh_count = fresh_keys.shape[0]
    query_heads = queries_now.reshape(row_count, KVH, group, HD)
    key_heads = cache_keys.reshape(row_count, positions, KVH, HD)
    value_heads = cache_values.reshape(row_count, positions, KVH, HD)
    fresh_key_heads = fresh_keys.reshape(fresh_count, row_count, KVH, HD)
    fresh_value_heads = fresh_values.reshape(fresh_count, row_count, KVH, HD)
    cached_scores = (
        jnp.einsum("rkgd,rpkd->rkgp", query_heads, key_heads, preferred_element_type=f32)
        * score_scale
    )
    fresh_scores = (
        jnp.einsum("rkgd,srkd->rkgs", query_heads, fresh_key_heads, preferred_element_type=f32)
        * score_scale
    )
    alive_mask = (jnp.arange(positions, dtype=jnp.int32)[None, :] < lengths[:, None])[
        :, None, None, :
    ]
    peak_score = jnp.maximum(
        jnp.max(jnp.where(alive_mask, cached_scores, neg_fill), axis=-1),
        jnp.max(fresh_scores, axis=-1),
    )
    cached_weights = jnp.where(alive_mask, jnp.exp(cached_scores - peak_score[..., None]), 0.0)
    fresh_weights = jnp.exp(fresh_scores - peak_score[..., None])
    weight_sum = jnp.sum(cached_weights, axis=-1) + jnp.sum(fresh_weights, axis=-1)
    cached_probs = (cached_weights / weight_sum[..., None]).astype(bf16)
    fresh_probs = (fresh_weights / weight_sum[..., None]).astype(bf16)
    output = jnp.einsum("rkgp,rpkd->rkgd", cached_probs, value_heads, preferred_element_type=f32)
    output = output + jnp.einsum(
        "rkgs,srkd->rkgd", fresh_probs, fresh_value_heads, preferred_element_type=f32
    )
    return output.astype(bf16).reshape(row_count, QH * HD)


def convert_kernel(cut_ref, gate_ref, up_ref, down_ref, inv_ref, scale_ref, *outs, step):
    cut = cut_ref[0]
    rows, width = gate_ref.shape[1], gate_ref.shape[2]
    span = min(width, 512)
    for j, (source, target) in enumerate(zip((gate_ref, up_ref, down_ref), outs)):
        for start in range(0, rows, step):
            which = (start >= cut).astype(jnp.int32)

            @pl.loop(0, width, step=span)
            def _(col):
                cols = pl.ds(pl.multiple_of(col, span), span)
                values = source[0, pl.ds(start, step), cols] * inv_ref[j, 0, pl.ds(which, 1), cols]
                spread = values * (2.0**20 + 1.0)
                normal = spread - (spread - values)
                small = (values + 24576.0) - 24576.0
                rounded = jnp.where(jnp.abs(values) < 2.0**-6, small, normal)
                restored = rounded * scale_ref[j, 0, pl.ds(which, 1), cols]
                target[0, pl.ds(start, step), cols] = restored.astype(bf16)


def convert(cut, masters, inverse, scales):
    experts, rows, width = masters[0].shape
    spec = pl.BlockSpec((1, rows, width), lambda e: (e, 0, 0))
    factor = pl.BlockSpec((3, 1, 2, width), lambda e: (0, e, 0, 0))
    count = 3 * experts * rows * width
    return pl.pallas_call(
        functools.partial(convert_kernel, step=math.gcd(rows, BLOCK)),
        grid=(experts,),
        in_specs=[pl.BlockSpec(memory_space=pltpu.SMEM), spec, spec, spec, factor, factor],
        out_specs=[spec] * 3,
        out_shape=[jax.ShapeDtypeStruct((experts, rows, width), bf16)] * 3,
        cost_estimate=pl.CostEstimate(
            flops=12 * count, bytes_accessed=6 * count, transcendentals=0
        ),
    )(cut, *masters, inverse, scales)


def group_max(value, axes, size):
    if size & (size - 1):
        return lax.pmax(value, axes)
    bit = 1
    while bit < size:
        other = lax.ppermute(value, axes, [(i, i ^ bit) for i in range(size)])
        value = jnp.maximum(value, other)
        bit *= 2
    return value


def gate_shares(routes, route_weights):
    total = jnp.sum(route_weights, axis=2)
    matches = routes[:, :, None, :] == jnp.arange(WIN, dtype=jnp.int32)[None, None, :, None]
    picked = jnp.sum(jnp.where(matches, route_weights[:, :, None, :], 0.0), axis=3)
    return picked / total[..., None]


def product(left, right, dims):
    return lax.dot_general(left, right, (dims, ((), ())), preferred_element_type=f32)


def local(sizes, hidden_in, queries, key_cache, value_cache, new_keys, new_values, lengths,
          routes, route_weights, norm_gain, gate_master, up_master, down_master, out_proj):
    fa, fb, cores, tps = sizes
    far, group, line = ("fa", "fb"), ("fb", "core", "tp"), fa * fb
    experts, shard, width = gate_master.shape
    tp_pos = lax.axis_index("tp")
    group_pos = lax.axis_index(group)
    rows = queries.shape[1]
    tiles = width // BLOCK
    masters = (gate_master, up_master, down_master)

    base = group_pos * shard
    first = base // BLOCK
    cut = (first + 1) * BLOCK - base
    count = fb * cores * tps * shard // BLOCK
    in_first = (jnp.arange(shard, dtype=jnp.int32) < cut)[None, :, None]

    def maxima(master):
        magnitude = jnp.abs(master)
        pair = [
            jnp.max(jnp.where(keep, magnitude, 0.0), axis=1) for keep in (in_first, ~in_first)
        ]
        return [jnp.max(side.reshape(experts, tiles, BLOCK), axis=2) for side in pair]

    sides = [maxima(master) for master in masters]
    lower = jnp.stack([side[0] for side in sides])[:, :, None, :]
    upper = jnp.stack([side[1] for side in sides])[:, :, None, :]
    places = jnp.arange(count, dtype=jnp.int32)[None, None, :, None]
    partial_max = jnp.where(places == first, lower, jnp.where(places == first + 1, upper, 0.0))
    block_max = group_max(partial_max, group, fb * cores * tps)
    scales = (block_max + epsilon) / fp_limit
    spread = jnp.stack(shifts(scales, "fa", fa))
    order = (lax.axis_index("fa") - jnp.arange(fa, dtype=jnp.int32)) % fa
    whole = jnp.moveaxis(spread[order], 0, 2).reshape(3, experts, fa * count, tiles)
    scale_log2 = jnp.log2(whole)

    padded = jnp.concatenate([scales, jnp.ones_like(scales[:, :, :1])], axis=2)
    own_scales = lax.dynamic_slice_in_dim(padded, first, 2, 2)
    inverse = (1.0 / own_scales) * (1.0 + 2.0**-22)
    own = convert(
        cut.astype(jnp.int32).reshape(1),
        masters,
        jnp.repeat(inverse, BLOCK, axis=3),
        jnp.repeat(own_scales, BLOCK, axis=3),
    )
    own = [matrix.reshape(experts * shard, width) for matrix in own]
    shared = [own]
    for s in range(1, cores):
        shared.append([shift(matrix, "core", cores, s) for matrix in own])

    shares = gate_shares(routes, route_weights)
    shares = jnp.stack(shifts(shares, far, line), axis=1)
    shares = shares.reshape(shares.shape[0], line, tps, rows, experts)
    shares = shares[:, :, (tp_pos - jnp.arange(tps, dtype=jnp.int32)) % tps]
    shares = shares.reshape(shares.shape[0], line * tps * rows, experts)

    def projection(step):
        heads = attention_rows(
            queries[step], key_cache, value_cache, new_keys[: step + 1], new_values[: step + 1],
            lengths,
        )
        part = out_proj.shape[0]
        pieces = [
            lax.dynamic_slice_in_dim(heads, (tp_pos + s) % tps * part, part, 1) for s in range(tps)
        ]
        pieces = pieces[:1] + [shift(pieces[s], "tp", tps, s) for s in range(1, tps)]
        total = product(jnp.concatenate(pieces), out_proj, ((1,), (0,)))
        total = total.reshape(tps, rows, width)
        result = total[0]
        for s in range(1, tps):
            result = result + shift(total[s].astype(bf16), "tp", tps, -s).astype(f32)
        return result

    def everyone(value):
        half = width // 2
        left, right = value[:, :half], value[:, half:]
        left = jnp.stack(shifts(left, far, line))
        right = jnp.stack(shifts(right, "tp", tps))
        left = jnp.stack(shifts(left, "tp", tps), axis=1)
        right = jnp.stack(shifts(right, far, line))
        return jnp.concatenate([left, right], axis=-1)

    def total_of(value):
        value = value.reshape(line, tps, rows, width)
        total = value[:, 0]
        for s in range(1, tps):
            total = total + shift(value[:, s].astype(bf16), "tp", tps, -s).astype(f32)
        result = total[0]
        for s in range(1, line):
            result = result + shift(total[s].astype(bf16), far, line, -s).astype(f32)
        return result

    def experts_of(mixed, share):
        values = mixed.reshape(line * tps * rows, width).astype(f32)
        inverse_rms = lax.rsqrt(jnp.mean(values * values, axis=1, keepdims=True) + epsilon)
        normed = (values * inverse_rms * norm_gain[None, :]).astype(bf16)
        factor = jnp.repeat(share, shard, axis=1)
        total = 0.0
        for gate, up, down in shared:
            gate_act = product(normed, gate, ((1,), (1,)))
            up_act = product(normed, up, ((1,), (1,)))
            act = (jax.nn.silu(gate_act) * up_act * factor).astype(bf16)
            total = total + product(act, down, ((1,), (0,)))
        return total

    current = lax.dynamic_slice_in_dim(hidden_in, tp_pos * rows, rows, 0).astype(f32)
    projected = [projection(step) for step in range(queries.shape[0])]
    for step, addend in enumerate(projected):
        mixed = (current + addend).astype(bf16)
        moe = total_of(experts_of(everyone(mixed), shares[step]))
        current = (mixed.astype(f32) + moe).astype(bf16).astype(f32)

    result = current.astype(bf16)
    part = width // tps
    pieces = [
        lax.dynamic_slice_in_dim(result, (tp_pos + s) % tps * part, part, 1) for s in range(tps)
    ]
    pieces = pieces[:1] + [shift(pieces[s], "tp", tps, s) for s in range(1, tps)]
    order = (tp_pos - jnp.arange(tps, dtype=jnp.int32)) % tps
    hidden_out = jnp.stack(pieces)[order].reshape(tps * rows, part)
    return (hidden_out, scale_log2)


def solution(mesh):
    fsdp, tps = mesh.shape["fsdp"], mesh.shape["tp"]
    cores = 2 if fsdp % 2 == 0 else 1

    def run(*args):
        shard = args[10].shape[1] // (fsdp * tps)
        devices = math.lcm(shard, BLOCK) // shard
        fb = fsdp // cores
        if devices % (cores * tps) == 0 and fb % (devices // (cores * tps)) == 0:
            fb = devices // (cores * tps)
        fa = fsdp // (cores * fb)
        sizes = (fa, fb, cores, tps)
        split = Mesh(mesh.devices.reshape(sizes), ("fa", "fb", "core", "tp"))
        f = ("fa", "fb", "core")
        every = f + ("tp",)
        in_specs = (
            P(f, None),
            P(None, every, None),
            P(every, None, None),
            P(every, None, None),
            P(None, every, None),
            P(None, every, None),
            P(every),
            P(None, f, None),
            P(None, f, None),
            P(),
            P(None, every, None),
            P(None, every, None),
            P(None, every, None),
            P("tp", None),
        )
        out_specs = (P(f, "tp"), P())
        body = jax.shard_map(
            functools.partial(local, sizes), mesh=split, in_specs=in_specs, out_specs=out_specs,
            check_vma=False,
        )
        return body(*args)

    return run
```

```python
import functools
import math

import jax
import jax.numpy as jnp
from jax import lax
from jax.experimental import pallas as pl
from jax.experimental.pallas import tpu as pltpu
from jax.sharding import Mesh, PartitionSpec as P


QH = 64
KVH = 4
HD = 128
BLOCK = 128
WIN = 8

neg_fill = -1e30
epsilon = 1e-06
fp_limit = 448.0
f32 = jnp.float32
bf16 = jnp.bfloat16


def swap(value, axis, size, distance):
    return lax.ppermute(value, axis, [(i, i ^ distance) for i in range(size)])


def swaps(value, axis, size):
    return [value] + [swap(value, axis, size, s) for s in range(1, size)]


def attention_rows(queries, cache_keys, cache_values, fresh_keys, fresh_values, lengths):
    steps, row_count = queries.shape[:2]
    positions = cache_keys.shape[1]
    group = QH // KVH
    score_scale = HD ** (-0.5)
    query_heads = queries.reshape(steps, row_count, KVH, group, HD)
    query_heads = jnp.transpose(query_heads, (1, 2, 0, 3, 4))
    query_heads = query_heads.reshape(row_count, KVH, steps * group, HD)
    key_heads = cache_keys.reshape(row_count, positions, KVH, HD)
    value_heads = cache_values.reshape(row_count, positions, KVH, HD)
    fresh_key_heads = fresh_keys.reshape(steps, row_count, KVH, HD)
    fresh_value_heads = fresh_values.reshape(steps, row_count, KVH, HD)
    cached_scores = (
        jnp.einsum("rkgd,rpkd->rkgp", query_heads, key_heads, preferred_element_type=f32)
        * score_scale
    )
    fresh_scores = (
        jnp.einsum("rkgd,srkd->rkgs", query_heads, fresh_key_heads, preferred_element_type=f32)
        * score_scale
    )
    alive_mask = (jnp.arange(positions, dtype=jnp.int32)[None, :] < lengths[:, None])[
        :, None, None, :
    ]
    step_of = jnp.arange(steps * group, dtype=jnp.int32) // group
    seen_mask = (jnp.arange(steps, dtype=jnp.int32)[None, :] <= step_of[:, None])[None, None]
    peak_score = jnp.maximum(
        jnp.max(jnp.where(alive_mask, cached_scores, neg_fill), axis=-1),
        jnp.max(jnp.where(seen_mask, fresh_scores, neg_fill), axis=-1),
    )
    cached_weights = jnp.where(alive_mask, jnp.exp(cached_scores - peak_score[..., None]), 0.0)
    fresh_weights = jnp.where(seen_mask, jnp.exp(fresh_scores - peak_score[..., None]), 0.0)
    weight_sum = jnp.sum(cached_weights, axis=-1) + jnp.sum(fresh_weights, axis=-1)
    cached_probs = (cached_weights / weight_sum[..., None]).astype(bf16)
    fresh_probs = (fresh_weights / weight_sum[..., None]).astype(bf16)
    output = jnp.einsum("rkgp,rpkd->rkgd", cached_probs, value_heads, preferred_element_type=f32)
    output = output + jnp.einsum(
        "rkgs,srkd->rkgd", fresh_probs, fresh_value_heads, preferred_element_type=f32
    )
    output = output.astype(bf16).reshape(row_count, KVH, steps, group * HD)
    return jnp.transpose(output, (2, 0, 1, 3)).reshape(steps, row_count, QH * HD)


def maxima_kernel(cut_ref, gate_ref, up_ref, down_ref, out_ref, *, step):
    cut = cut_ref[0]
    rows, width = gate_ref.shape[1], gate_ref.shape[2]
    for j, source in enumerate((gate_ref, up_ref, down_ref)):
        pair = [jnp.zeros((step, width), f32)] * 2
        for start in range(0, rows, step):
            values = jnp.abs(source[0, pl.ds(start, step), :])
            inside = start < cut
            pair[0] = jnp.maximum(pair[0], jnp.where(inside, values, 0.0))
            pair[1] = jnp.maximum(pair[1], jnp.where(inside, 0.0, values))
        for side in range(2):
            out_ref[j, 0, pl.ds(side, 1), :] = jnp.max(pair[side], axis=0, keepdims=True)


def maxima(cut, masters):
    experts, rows, width = masters[0].shape
    spec = pl.BlockSpec((1, rows, width), lambda e: (e, 0, 0))
    count = 3 * experts * rows * width
    return pl.pallas_call(
        functools.partial(maxima_kernel, step=math.gcd(rows, BLOCK)),
        grid=(experts,),
        in_specs=[pl.BlockSpec(memory_space=pltpu.SMEM), spec, spec, spec],
        out_specs=pl.BlockSpec((3, 1, 2, width), lambda e: (0, e, 0, 0)),
        out_shape=jax.ShapeDtypeStruct((3, experts, 2, width), f32),
        cost_estimate=pl.CostEstimate(flops=4 * count, bytes_accessed=4 * count, transcendentals=0),
    )(cut, *masters)


def convert_kernel(cut_ref, gate_ref, up_ref, down_ref, scale_ref, *refs, step):
    outs, inv_ref = refs[:3], refs[3]
    cut = cut_ref[0]
    rows, width = gate_ref.shape[1], gate_ref.shape[2]
    span = min(width, 2048)
    for j in range(3):
        inv_ref[j] = (1.0 / scale_ref[j, 0]) * (1.0 + 2.0**-22)
    for j, (source, target) in enumerate(zip((gate_ref, up_ref, down_ref), outs)):
        for start in range(0, rows, step):
            which = (start >= cut).astype(jnp.int32)

            @pl.loop(0, width, step=span)
            def _(col):
                cols = pl.ds(pl.multiple_of(col, span), span)
                values = source[0, pl.ds(start, step), cols] * inv_ref[j, pl.ds(which, 1), cols]
                spread = values * (2.0**20 + 1.0)
                normal = spread - (spread - values)
                small = (values + 24576.0) - 24576.0
                rounded = jnp.where(jnp.abs(values) < 2.0**-6, small, normal)
                restored = rounded * scale_ref[j, 0, pl.ds(which, 1), cols]
                target[0, pl.ds(start, step), cols] = restored.astype(bf16)


def convert(cut, masters, scales):
    experts, rows, width = masters[0].shape
    spec = pl.BlockSpec((1, rows, width), lambda e: (e, 0, 0))
    factor = pl.BlockSpec((3, 1, 2, width), lambda e: (0, e, 0, 0))
    count = 3 * experts * rows * width
    return pl.pallas_call(
        functools.partial(convert_kernel, step=math.gcd(rows, BLOCK)),
        grid=(experts,),
        in_specs=[pl.BlockSpec(memory_space=pltpu.SMEM), spec, spec, spec, factor],
        out_specs=[spec] * 3,
        out_shape=[jax.ShapeDtypeStruct((experts, rows, width), bf16)] * 3,
        scratch_shapes=[pltpu.VMEM((3, 2, width), f32)],
        cost_estimate=pl.CostEstimate(
            flops=12 * count, bytes_accessed=6 * count, transcendentals=0
        ),
    )(cut, *masters, scales)


def group_max(value, axes, size):
    if size & (size - 1):
        return lax.pmax(value, axes)
    bit = 1
    while bit < size:
        other = lax.ppermute(value, axes, [(i, i ^ bit) for i in range(size)])
        value = jnp.maximum(value, other)
        bit *= 2
    return value


def gate_shares(routes, route_weights):
    total = jnp.sum(route_weights, axis=2)
    matches = routes[:, :, None, :] == jnp.arange(WIN, dtype=jnp.int32)[None, None, :, None]
    picked = jnp.sum(jnp.where(matches, route_weights[:, :, None, :], 0.0), axis=3)
    return picked / total[..., None]


def product(left, right, dims):
    return lax.dot_general(left, right, (dims, ((), ())), preferred_element_type=f32)


def expert_kernel(line, tps, cores, last, place_ref, gain_ref, factor_ref, *refs):
    lefts, refs = refs[:tps], refs[tps:]
    rights, refs = refs[:line], refs[line:]
    weights, refs = refs[: 3 * cores], refs[3 * cores :]
    outs, (rows_ref, act_ref, gate_ref, up_ref, down_ref, sems) = refs[:tps], refs[tps:]
    hidden, width = weights[0].shape
    rows, half = lefts[0].shape[1:]
    copies = []
    for j, target in enumerate((gate_ref, up_ref, down_ref)):
        for c in range(cores):
            spot = pl.ds(c * hidden, hidden)
            copies.append(
                pltpu.make_async_copy(weights[3 * c + j], target.at[spot], sems.at[j * cores + c])
            )
    for copy in copies:
        copy.start()

    for z in range(line):
        for t in range(tps):
            spot = pl.ds((z * tps + t) * rows, rows)
            rows_ref[spot, :half] = lefts[t][z]
            rows_ref[spot, half:] = rights[z][t]

    @pl.loop(0, line * tps * rows, step=16)
    def _(start):
        spot = pl.ds(pl.multiple_of(start, 16), 16)
        values = rows_ref[spot, :].astype(f32)
        mean = jnp.sum(values * values, axis=1, keepdims=True) * (1.0 / width)
        rows_ref[spot, :] = (values * lax.rsqrt(mean + epsilon) * gain_ref[...]).astype(bf16)

    for copy in copies[: 2 * cores]:
        copy.wait()
    chunk = BLOCK if hidden % BLOCK == 0 else hidden
    total = cores * hidden
    for at in range(0, total, chunk):
        pair = jnp.concatenate([gate_ref[pl.ds(at, chunk), :], up_ref[pl.ds(at, chunk), :]])
        both = product(rows_ref[...], pair, ((1,), (1,)))
        gate, up = both[:, :chunk], both[:, chunk:]
        inside = pl.ds(at % hidden, chunk)
        act = gate / (1.0 + jnp.exp(-gate)) * up * factor_ref[:, inside]
        act_ref[at // chunk] = act.astype(bf16)

    for copy in copies[2 * cores :]:
        copy.wait()
    act = jnp.concatenate([act_ref[i] for i in range(total // chunk)], axis=1)
    if last:
        place = place_ref[0]
        part = width // tps
        for r in range(tps):
            cols = pl.ds(pl.multiple_of((place ^ r) * part, part), part)
            result = product(act, down_ref[:, cols], ((1,), (0,))).astype(bf16)
            for z in range(line):
                for t in range(tps):
                    start = (z * tps + t) * rows
                    outs[r][z, place ^ t] = result[start : start + rows]
    else:
        span = min(width, 512)

        @pl.loop(0, width, step=span)
        def _(col):
            cols = pl.ds(pl.multiple_of(col, span), span)
            result = product(act, down_ref[:, cols], ((1,), (0,))).astype(bf16)
            for z in range(line):
                for t in range(tps):
                    start = (z * tps + t) * rows
                    outs[t][z, :, cols] = result[start : start + rows]


def experts_of(place, gain, factor, lefts, rights, shared, last):
    tps, line, cores = len(lefts), len(rights), len(shared)
    rows, half = lefts[0].shape[1:]
    width = half + rights[0].shape[2]
    hidden = shared[0][0].shape[0]
    count = line * tps * rows
    chunk = BLOCK if hidden % BLOCK == 0 else hidden
    vmem = pl.BlockSpec(memory_space=pltpu.VMEM)
    hbm = pl.BlockSpec(memory_space=pltpu.HBM)
    shape = (line, tps, rows, width // tps) if last else (line, rows, width)
    return pl.pallas_call(
        functools.partial(expert_kernel, line, tps, cores, last),
        in_specs=[pl.BlockSpec(memory_space=pltpu.SMEM)]
        + [vmem] * (2 + tps + line)
        + [hbm] * (3 * cores),
        out_specs=[vmem] * tps,
        out_shape=[jax.ShapeDtypeStruct(shape, bf16)] * tps,
        scratch_shapes=[
            pltpu.VMEM((count, width), bf16),
            pltpu.VMEM((cores * hidden // chunk, count, chunk), bf16),
            pltpu.VMEM((cores * hidden, width), bf16),
            pltpu.VMEM((cores * hidden, width), bf16),
            pltpu.VMEM((cores * hidden, width), bf16),
            pltpu.SemaphoreType.DMA((3 * cores,)),
        ],
        cost_estimate=pl.CostEstimate(
            flops=6 * count * width * cores * hidden,
            bytes_accessed=6 * cores * hidden * width,
            transcendentals=count * cores * hidden,
        ),
    )(place, gain, factor, *lefts, *rights, *[m for matrices in shared for m in matrices])


def local(sizes, hidden_in, queries, key_cache, value_cache, new_keys, new_values, lengths,
          routes, route_weights, norm_gain, gate_master, up_master, down_master, out_proj):
    fa, fb, cores, tps = sizes
    far, group, line = ("fa", "fb"), ("fb", "core", "tp"), fa * fb
    experts, shard, width = gate_master.shape
    tp_pos = lax.axis_index("tp")
    group_pos = lax.axis_index(group)
    rows = queries.shape[1]
    tiles = width // BLOCK
    masters = (gate_master, up_master, down_master)

    base = group_pos * shard
    first = base // BLOCK
    cut = (first + 1) * BLOCK - base
    count = fb * cores * tps * shard // BLOCK
    cut = cut.astype(jnp.int32).reshape(1)
    sides = maxima(cut, masters)
    sides = jnp.max(sides.reshape(3, experts, 2, tiles, BLOCK), axis=4)
    places = jnp.arange(count, dtype=jnp.int32)[None, None, :, None]
    partial_max = jnp.where(
        places == first,
        sides[:, :, :1],
        jnp.where(places == first + 1, sides[:, :, 1:], 0.0),
    )
    partial_max, queries = lax.optimization_barrier((partial_max, queries))
    block_max = group_max(partial_max, group, fb * cores * tps)
    scales = (block_max + epsilon) / fp_limit

    steps = queries.shape[0]
    heads = attention_rows(queries, key_cache, value_cache, new_keys, new_values, lengths)
    part = out_proj.shape[0]
    pieces = [lax.dynamic_slice_in_dim(heads, (tp_pos ^ s) * part, part, 2) for s in range(tps)]
    pieces = [pieces[0]] + [swap(pieces[s], "tp", tps, s) for s in range(1, tps)]

    padded = jnp.concatenate([scales, jnp.ones_like(scales[:, :, :1])], axis=2)
    own_scales = lax.dynamic_slice_in_dim(padded, first, 2, 2)
    own = convert(cut, masters, jnp.repeat(own_scales, BLOCK, axis=3))
    own = [matrix.reshape(experts * shard, width) for matrix in own]
    shared = [own]
    for s in range(1, cores):
        shared.append([swap(matrix, "core", cores, s) for matrix in own])

    shares = gate_shares(routes, route_weights).reshape(-1, experts)
    packet = jnp.concatenate(
        [scales.reshape(-1, tiles), jnp.pad(shares, ((0, 0), (0, tiles - experts)))]
    )
    packet, pieces[0] = lax.optimization_barrier((packet, pieces[0]))
    packets = swaps(packet, far, line)
    cells = 3 * experts * count
    spread = jnp.stack([packets[a * fb][:cells] for a in range(fa)])
    whole = spread[lax.axis_index("fa") ^ jnp.arange(fa, dtype=jnp.int32)]
    whole = jnp.moveaxis(whole.reshape(fa, 3, experts, count, tiles), 0, 2)
    scale_log2 = jnp.log2(whole.reshape(3, experts, fa * count, tiles))
    shares = jnp.stack([packet[cells:, :experts] for packet in packets])
    shares = jnp.moveaxis(shares.reshape(line, steps, tps, rows, experts), 1, 0)
    order = tp_pos ^ jnp.arange(tps, dtype=jnp.int32)
    shares = shares[:, :, order].reshape(steps, line * tps * rows, experts)
    factors = jnp.repeat(shares, shard, axis=2)

    joined = jnp.concatenate([piece[None] for piece in pieces])
    joined, own[0] = lax.optimization_barrier((joined, own[0]))
    total = product(joined.reshape(-1, part), out_proj, ((1,), (0,)))
    total = total.reshape(tps, steps, rows, width)

    def projection(total, step):
        result = total[0, step]
        for s in range(1, tps):
            result = result + swap(total[s, step].astype(bf16), "tp", tps, s).astype(f32)
        return result

    def everyone(value):
        half = width * 5 // 8 // BLOCK * BLOCK
        left = jnp.stack(swaps(value[:, :half], far, line))
        right = jnp.stack(swaps(value[:, half:], "tp", tps))
        return swaps(left, "tp", tps), swaps(right, far, line)

    def total_of(parts):
        total = parts[0].astype(f32)
        for s in range(1, tps):
            total = total + swap(parts[s], "tp", tps, s).astype(f32)
        result = total[0]
        for s in range(1, line):
            result = result + swap(total[s].astype(bf16), far, line, s).astype(f32)
        return result

    place = tp_pos.astype(jnp.int32).reshape(1)
    gain = norm_gain.reshape(1, width)
    current = lax.dynamic_slice_in_dim(hidden_in, tp_pos * rows, rows, 0).astype(f32)
    for step in range(steps):
        last = step == steps - 1
        addend = projection(total, step)
        mixed = (current + addend).astype(bf16)
        lefts, rights = everyone(mixed)
        if not last:
            total, lefts[0] = lax.optimization_barrier((total, lefts[0]))
        parts = experts_of(place, gain, factors[step], lefts, rights, shared, last)
        moe = total_of(parts)
        if last:
            own_rows = jnp.concatenate([jnp.stack([left[0] for left in lefts]), rights[0]], axis=2)
            part = width // tps
            mixed = lax.dynamic_slice_in_dim(own_rows, tp_pos * part, part, 2)[order]
        current = (mixed.astype(f32) + moe).astype(bf16).astype(f32)
    hidden_out = current.astype(bf16).reshape(tps * rows, width // tps)
    return (hidden_out, scale_log2)


def solution(mesh):
    fsdp, tps = mesh.shape["fsdp"], mesh.shape["tp"]
    cores = 2 if fsdp % 2 == 0 else 1

    def run(*args):
        shard = args[10].shape[1] // (fsdp * tps)
        devices = math.lcm(shard, BLOCK) // shard
        fb = fsdp // cores
        if devices % (cores * tps) == 0 and fb % (devices // (cores * tps)) == 0:
            fb = devices // (cores * tps)
        fa = fsdp // (cores * fb)
        sizes = (fa, fb, cores, tps)
        split = Mesh(mesh.devices.reshape(sizes), ("fa", "fb", "core", "tp"))
        f = ("fa", "fb", "core")
        every = f + ("tp",)
        in_specs = (
            P(f, None),
            P(None, every, None),
            P(every, None, None),
            P(every, None, None),
            P(None, every, None),
            P(None, every, None),
            P(every),
            P(None, f, None),
            P(None, f, None),
            P(),
            P(None, every, None),
            P(None, every, None),
            P(None, every, None),
            P("tp", None),
        )
        out_specs = (P(f, "tp"), P())
        body = jax.shard_map(
            functools.partial(local, sizes), mesh=split, in_specs=in_specs, out_specs=out_specs,
            check_vma=False,
        )
        return body(*args)

    return run
```

```python
import functools
import math

import jax
import jax.numpy as jnp
from jax import lax
from jax.experimental import pallas as pl
from jax.experimental.pallas import tpu as pltpu
from jax.sharding import Mesh, PartitionSpec as P


QH = 64
KVH = 4
HD = 128
BLOCK = 128
WIN = 8

neg_fill = -1e30
epsilon = 1e-06
fp_limit = 448.0
f32 = jnp.float32
bf16 = jnp.bfloat16


def swap(value, axis, size, distance):
    return lax.ppermute(value, axis, [(i, i ^ distance) for i in range(size)])


def swaps(value, axis, size):
    return [value] + [swap(value, axis, size, s) for s in range(1, size)]


def attention_rows(queries, cache_keys, cache_values, fresh_keys, fresh_values, lengths):
    steps, row_count = queries.shape[:2]
    positions = cache_keys.shape[1]
    group = QH // KVH
    score_scale = HD ** (-0.5)
    query_heads = queries.reshape(steps, row_count, KVH, group, HD)
    query_heads = jnp.transpose(query_heads, (1, 2, 0, 3, 4))
    query_heads = query_heads.reshape(row_count, KVH, steps * group, HD)
    key_heads = cache_keys.reshape(row_count, positions, KVH, HD)
    value_heads = cache_values.reshape(row_count, positions, KVH, HD)
    fresh_key_heads = fresh_keys.reshape(steps, row_count, KVH, HD)
    fresh_value_heads = fresh_values.reshape(steps, row_count, KVH, HD)
    cached_scores = (
        jnp.einsum("rkgd,rpkd->rkgp", query_heads, key_heads, preferred_element_type=f32)
        * score_scale
    )
    fresh_scores = (
        jnp.einsum("rkgd,srkd->rkgs", query_heads, fresh_key_heads, preferred_element_type=f32)
        * score_scale
    )
    alive_mask = (jnp.arange(positions, dtype=jnp.int32)[None, :] < lengths[:, None])[
        :, None, None, :
    ]
    step_of = jnp.arange(steps * group, dtype=jnp.int32) // group
    seen_mask = (jnp.arange(steps, dtype=jnp.int32)[None, :] <= step_of[:, None])[None, None]
    peak_score = jnp.maximum(
        jnp.max(jnp.where(alive_mask, cached_scores, neg_fill), axis=-1),
        jnp.max(jnp.where(seen_mask, fresh_scores, neg_fill), axis=-1),
    )
    cached_weights = jnp.where(alive_mask, jnp.exp(cached_scores - peak_score[..., None]), 0.0)
    fresh_weights = jnp.where(seen_mask, jnp.exp(fresh_scores - peak_score[..., None]), 0.0)
    weight_sum = jnp.sum(cached_weights, axis=-1) + jnp.sum(fresh_weights, axis=-1)
    cached_probs = (cached_weights / weight_sum[..., None]).astype(bf16)
    fresh_probs = (fresh_weights / weight_sum[..., None]).astype(bf16)
    output = jnp.einsum("rkgp,rpkd->rkgd", cached_probs, value_heads, preferred_element_type=f32)
    output = output + jnp.einsum(
        "rkgs,srkd->rkgd", fresh_probs, fresh_value_heads, preferred_element_type=f32
    )
    output = output.astype(bf16).reshape(row_count, KVH, steps, group * HD)
    return jnp.transpose(output, (2, 0, 1, 3)).reshape(steps, row_count, QH * HD)


def maxima_kernel(cut_ref, gate_ref, up_ref, down_ref, out_ref, *, step):
    cut = cut_ref[0]
    rows, width = gate_ref.shape[1], gate_ref.shape[2]
    span = min(width, 512)
    for j, source in enumerate((gate_ref, up_ref, down_ref)):

        @pl.loop(0, width, step=span)
        def _(col):
            cols = pl.ds(pl.multiple_of(col, span), span)
            pair = [jnp.zeros((min(step, 8), span), f32)] * 2
            for start in range(0, rows, step):
                values = jnp.abs(source[0, pl.ds(start, step), cols])
                if step > 8:
                    values = jnp.max(values.reshape(step // 8, 8, span), axis=0)
                inside = start < cut
                pair[0] = jnp.maximum(pair[0], jnp.where(inside, values, 0.0))
                pair[1] = jnp.maximum(pair[1], jnp.where(inside, 0.0, values))
            for side in range(2):
                out_ref[j, 0, pl.ds(side, 1), cols] = jnp.max(pair[side], axis=0, keepdims=True)


def maxima(cut, masters):
    experts, rows, width = masters[0].shape
    spec = pl.BlockSpec((1, rows, width), lambda e: (e, 0, 0))
    count = 3 * experts * rows * width
    return pl.pallas_call(
        functools.partial(maxima_kernel, step=math.gcd(rows, BLOCK)),
        grid=(experts,),
        in_specs=[pl.BlockSpec(memory_space=pltpu.SMEM), spec, spec, spec],
        out_specs=pl.BlockSpec((3, 1, 2, width), lambda e: (0, e, 0, 0)),
        out_shape=jax.ShapeDtypeStruct((3, experts, 2, width), f32),
        cost_estimate=pl.CostEstimate(flops=4 * count, bytes_accessed=4 * count, transcendentals=0),
    )(cut, *masters)


def convert_kernel(cut_ref, gain_ref, gate_ref, up_ref, down_ref, scale_ref, *refs, step):
    outs, (inv_ref, back_ref) = refs[:3], refs[3:]
    cut = cut_ref[0]
    rows, width = gate_ref.shape[1], gate_ref.shape[2]
    span = min(width, 512)
    for j in range(3):
        inv_ref[j] = (1.0 / scale_ref[j, 0]) * (1.0 + 2.0**-22)
        back_ref[j] = scale_ref[j, 0] * gain_ref[...] if j < 2 else scale_ref[j, 0]
    for j, (source, target) in enumerate(zip((gate_ref, up_ref, down_ref), outs)):

        @pl.loop(0, width, step=span)
        def _(col):
            cols = pl.ds(pl.multiple_of(col, span), span)
            low = min(step, 8)
            sides = [
                [jnp.broadcast_to(ref[j, pl.ds(side, 1), cols], (low, span)) for side in range(2)]
                for ref in (inv_ref, back_ref)
            ]
            for start in range(0, rows, step):
                inside = start < cut
                inv, back = [jnp.where(inside, side[0], side[1])[None] for side in sides]
                values = source[0, pl.ds(start, step), cols].reshape(step // low, low, span) * inv
                spread = values * (2.0**20 + 1.0)
                normal = spread - (spread - values)
                small = (values + 24576.0) - 24576.0
                rounded = jnp.where(jnp.abs(values) < 2.0**-6, small, normal)
                restored = (rounded * back).reshape(step, span)
                target[0, pl.ds(start, step), cols] = restored.astype(bf16)


def convert(cut, gain, masters, scales):
    experts, rows, width = masters[0].shape
    spec = pl.BlockSpec((1, rows, width), lambda e: (e, 0, 0))
    factor = pl.BlockSpec((3, 1, 2, width), lambda e: (0, e, 0, 0))
    count = 3 * experts * rows * width
    return pl.pallas_call(
        functools.partial(convert_kernel, step=math.gcd(rows, BLOCK)),
        grid=(experts,),
        in_specs=[
            pl.BlockSpec(memory_space=pltpu.SMEM),
            pl.BlockSpec((1, width), lambda e: (0, 0)),
            spec,
            spec,
            spec,
            factor,
        ],
        out_specs=[spec] * 3,
        out_shape=[jax.ShapeDtypeStruct((experts, rows, width), bf16)] * 3,
        scratch_shapes=[pltpu.VMEM((3, 2, width), f32)] * 2,
        cost_estimate=pl.CostEstimate(
            flops=12 * count, bytes_accessed=6 * count, transcendentals=0
        ),
    )(cut, gain, *masters, scales)


def group_max(value, axes, size):
    if size & (size - 1):
        return lax.pmax(value, axes)
    bit = 1
    while bit < size:
        other = lax.ppermute(value, axes, [(i, i ^ bit) for i in range(size)])
        value = jnp.maximum(value, other)
        bit *= 2
    return value


def gate_shares(routes, route_weights):
    total = jnp.sum(route_weights, axis=2)
    matches = routes[:, :, None, :] == jnp.arange(WIN, dtype=jnp.int32)[None, None, :, None]
    picked = jnp.sum(jnp.where(matches, route_weights[:, :, None, :], 0.0), axis=3)
    return picked / total[..., None]


def product(left, right, dims):
    return lax.dot_general(left, right, (dims, ((), ())), preferred_element_type=f32)


def expert_kernel(line, tps, cores, last, experts, place_ref, *refs):
    lefts, refs = refs[:tps], refs[tps:]
    rights, refs = refs[:line], refs[line:]
    weights, refs = refs[: 3 * cores], refs[3 * cores :]
    outs, refs = refs[:tps], refs[tps:]
    others, (rows_ref, extra_ref, act_ref, gate_ref, up_ref, down_ref, sems) = refs[:line], refs[line:]
    hidden, width = weights[0].shape
    rows, half = lefts[0].shape[1:]
    copies = []
    for j, target in enumerate((gate_ref, up_ref, down_ref)):
        for c in range(cores):
            spot = pl.ds(c * hidden, hidden)
            copies.append(
                pltpu.make_async_copy(weights[3 * c + j], target.at[spot], sems.at[j * cores + c])
            )
    for copy in copies:
        copy.start()

    for z in range(line):
        for t in range(tps):
            spot = pl.ds((z * tps + t) * rows, rows)
            rows_ref[spot, :half] = lefts[t][z]
            rows_ref[spot, half:] = rights[z][t, :, : width - half]
            extra_ref[spot, :] = rights[z][t, :, width - half :]

    lanes = extra_ref.shape[1]
    entry = lax.broadcasted_iota(jnp.int32, (lanes, hidden), 0)
    owner = lax.broadcasted_iota(jnp.int32, (lanes, hidden), 1) // (hidden // experts)
    chosen = ((entry == owner) | (entry == owner + experts)).astype(f32).astype(bf16)
    factor = product(extra_ref[...], chosen, ((1,), (0,)))
    chunk = BLOCK if hidden % BLOCK == 0 else hidden
    entry = lax.broadcasted_iota(jnp.int32, (lanes, chunk), 0)
    alone = ((entry == 2 * experts) | (entry == 2 * experts + 1)).astype(f32).astype(bf16)
    inverse_rms = product(extra_ref[...], alone, ((1,), (0,)))

    for copy in copies[: 2 * cores]:
        copy.wait()
    total = cores * hidden
    for at in range(0, total, chunk):
        pair = jnp.concatenate([gate_ref[pl.ds(at, chunk), :], up_ref[pl.ds(at, chunk), :]])
        both = product(rows_ref[...], pair, ((1,), (1,)))
        gate, up = both[:, :chunk] * inverse_rms, both[:, chunk:]
        inside = at % hidden
        act = gate / (1.0 + jnp.exp(-gate)) * up * factor[:, inside : inside + chunk]
        act_ref[at // chunk] = act.astype(bf16)

    for copy in copies[2 * cores :]:
        copy.wait()
    act = jnp.concatenate([act_ref[i] for i in range(total // chunk)], axis=1)
    if last:
        place = place_ref[0]
        part = width // tps
        first = outs[0].shape[-1]
        for r in range(tps):
            cols = pl.ds(pl.multiple_of((place ^ r) * part, part), part)
            result = product(act, down_ref[:, cols], ((1,), (0,))).astype(bf16)
            for z in range(line):
                for t in range(tps):
                    start = (z * tps + t) * rows
                    outs[r][z, place ^ t] = result[start : start + rows, :first]
                    others[z][r, place ^ t] = result[start : start + rows, first:]
    else:
        first = outs[0].shape[-1]
        span = math.gcd(first, 512)
        for begin, end in ((0, first), (first, width)):

            @pl.loop(begin, end, step=span)
            def _(col):
                cols = pl.ds(pl.multiple_of(col, span), span)
                result = product(act, down_ref[:, cols], ((1,), (0,))).astype(bf16)
                spot = pl.ds(pl.multiple_of(col - begin, span), span)
                for z in range(line):
                    for t in range(tps):
                        start = (z * tps + t) * rows
                        target = outs[t].at[z] if begin == 0 else others[z].at[t]
                        target[:, spot] = result[start : start + rows]


def experts_of(place, experts, lefts, rights, shared, last):
    tps, line, cores = len(lefts), len(rights), len(shared)
    rows, half = lefts[0].shape[1:]
    hidden, width = shared[0][0].shape
    extra = rights[0].shape[2] - (width - half)
    count = line * tps * rows
    chunk = BLOCK if hidden % BLOCK == 0 else hidden
    vmem = pl.BlockSpec(memory_space=pltpu.VMEM)
    hbm = pl.BlockSpec(memory_space=pltpu.HBM)
    part = width // tps if last else width
    first = part * 3 // 4 // BLOCK * BLOCK
    middle = (tps, rows) if last else (rows,)
    shapes = [(line, *middle, first)] * tps + [(tps, *middle, part - first)] * line
    return pl.pallas_call(
        functools.partial(expert_kernel, line, tps, cores, last, experts),
        in_specs=[pl.BlockSpec(memory_space=pltpu.SMEM)]
        + [vmem] * (tps + line)
        + [hbm] * (3 * cores),
        out_specs=[vmem] * len(shapes),
        out_shape=[jax.ShapeDtypeStruct(shape, bf16) for shape in shapes],
        scratch_shapes=[
            pltpu.VMEM((count, width), bf16),
            pltpu.VMEM((count, extra), bf16),
            pltpu.VMEM((cores * hidden // chunk, count, chunk), bf16),
            pltpu.VMEM((cores * hidden, width), bf16),
            pltpu.VMEM((cores * hidden, width), bf16),
            pltpu.VMEM((cores * hidden, width), bf16),
            pltpu.SemaphoreType.DMA((3 * cores,)),
        ],
        cost_estimate=pl.CostEstimate(
            flops=6 * count * width * cores * hidden,
            bytes_accessed=6 * cores * hidden * width,
            transcendentals=count * cores * hidden,
        ),
    )(place, *lefts, *rights, *[m for matrices in shared for m in matrices])


def local(sizes, hidden_in, queries, key_cache, value_cache, new_keys, new_values, lengths,
          routes, route_weights, norm_gain, gate_master, up_master, down_master, out_proj):
    fa, fb, cores, tps = sizes
    far, group, line = ("fa", "fb"), ("fb", "core", "tp"), fa * fb
    experts, shard, width = gate_master.shape
    tp_pos = lax.axis_index("tp")
    group_pos = lax.axis_index(group)
    rows = queries.shape[1]
    tiles = width // BLOCK
    masters = (gate_master, up_master, down_master)

    base = group_pos * shard
    first = base // BLOCK
    cut = (first + 1) * BLOCK - base
    count = fb * cores * tps * shard // BLOCK
    cut = cut.astype(jnp.int32).reshape(1)
    sides = maxima(cut, masters)
    sides = jnp.max(sides.reshape(3, experts, 2, tiles, BLOCK), axis=4)
    places = jnp.arange(count, dtype=jnp.int32)[None, None, :, None]
    partial_max = jnp.where(
        places == first,
        sides[:, :, :1],
        jnp.where(places == first + 1, sides[:, :, 1:], 0.0),
    )
    partial_max, queries = lax.optimization_barrier((partial_max, queries))
    block_max = group_max(partial_max, group, fb * cores * tps)
    scales = (block_max + epsilon) / fp_limit

    steps = queries.shape[0]
    heads = attention_rows(queries, key_cache, value_cache, new_keys, new_values, lengths)
    part = out_proj.shape[0]
    pieces = [lax.dynamic_slice_in_dim(heads, (tp_pos ^ s) * part, part, 2) for s in range(tps)]
    pieces = [pieces[0]] + [swap(pieces[s], "tp", tps, s) for s in range(1, tps)]

    joined = jnp.concatenate([piece[None] for piece in pieces])
    total = product(joined.reshape(-1, part), out_proj, ((1,), (0,)))
    total = total.reshape(tps, steps, rows, width)

    padded = jnp.concatenate([scales, jnp.ones_like(scales[:, :, :1])], axis=2)
    own_scales = lax.dynamic_slice_in_dim(padded, first, 2, 2)
    spread_scales = swaps(scales, "fa", fa)
    own_scales, total, spread_scales = lax.optimization_barrier((own_scales, total, spread_scales))
    addends = total[0]
    for s in range(1, tps):
        addends = addends + swap(total[s].astype(bf16), "tp", tps, s).astype(f32)
    spread = jnp.repeat(own_scales, BLOCK, axis=3)
    own = list(convert(cut, norm_gain.reshape(1, width), masters, spread))
    addends, own[0] = lax.optimization_barrier((addends, own[0]))
    own = [matrix.reshape(experts * shard, width) for matrix in own]
    shared = [own]
    for s in range(1, cores):
        shared.append([swap(matrix, "core", cores, s) for matrix in own])

    shares = gate_shares(routes, route_weights)
    shares = lax.dynamic_slice_in_dim(shares, tp_pos * rows, rows, 1)
    order = tp_pos ^ jnp.arange(tps, dtype=jnp.int32)

    def beside(mixed, share):
        values = mixed.astype(f32)
        inverse = lax.rsqrt(jnp.mean(values * values, axis=1, keepdims=True) + epsilon)
        share = share * inverse
        parts = []
        for value in (share, inverse):
            high = lax.reduce_precision(value, 8, 7)
            parts += [high, value - high]
        parts = jnp.concatenate(parts, axis=1)
        return jnp.pad(parts, ((0, 0), (0, BLOCK - parts.shape[1]))).astype(bf16)

    half = width * 3 // 4 // BLOCK * BLOCK

    def everyone(mixed, share):
        left = jnp.stack(swaps(mixed[:, :half], far, line))
        right = jnp.concatenate([mixed[:, half:], beside(mixed, share)], axis=1)
        right = jnp.stack(swaps(right, "tp", tps))
        return swaps(left, "tp", tps), swaps(right, far, line)

    def summed(parts, axis):
        parts = list(parts)
        total = parts[0].astype(f32)
        for s in range(1, len(parts)):
            total = total + swap(parts[s].astype(bf16), axis, len(parts), s).astype(f32)
        return total

    def total_of(parts):
        left = summed(summed(parts[:tps], "tp"), far)
        right = summed(summed(parts[tps:], far), "tp")
        return jnp.concatenate([left, right], axis=-1)

    place = tp_pos.astype(jnp.int32).reshape(1)
    current = lax.dynamic_slice_in_dim(hidden_in, tp_pos * rows, rows, 0).astype(f32)
    for step in range(steps):
        last = step == steps - 1
        mixed = (current + addends[step]).astype(bf16)
        lefts, rights = everyone(mixed, shares[step])
        parts = list(experts_of(place, experts, lefts, rights, shared, last))
        moe = total_of(parts)
        if last:
            own_rows = jnp.concatenate([jnp.stack([left[0] for left in lefts]), rights[0][..., : width - half]], axis=2)
            part = width // tps
            mixed = lax.dynamic_slice_in_dim(own_rows, tp_pos * part, part, 2)[order]
        current = (mixed.astype(f32) + moe).astype(bf16).astype(f32)
    spread = jnp.stack(spread_scales)
    spread = spread[lax.axis_index("fa") ^ jnp.arange(fa, dtype=jnp.int32)]
    scale_log2 = jnp.log2(jnp.moveaxis(spread, 0, 2).reshape(3, experts, fa * count, tiles))
    hidden_out = current.astype(bf16).reshape(tps * rows, width // tps)
    return (hidden_out, scale_log2)


def solution(mesh):
    fsdp, tps = mesh.shape["fsdp"], mesh.shape["tp"]
    cores = 2 if fsdp % 2 == 0 else 1

    def run(*args):
        shard = args[10].shape[1] // (fsdp * tps)
        devices = math.lcm(shard, BLOCK) // shard
        fb = fsdp // cores
        if devices % (cores * tps) == 0 and fb % (devices // (cores * tps)) == 0:
            fb = devices // (cores * tps)
        fa = fsdp // (cores * fb)
        sizes = (fa, fb, cores, tps)
        split = Mesh(mesh.devices.reshape(sizes), ("fa", "fb", "core", "tp"))
        f = ("fa", "fb", "core")
        every = f + ("tp",)
        in_specs = (
            P(f, None),
            P(None, every, None),
            P(every, None, None),
            P(every, None, None),
            P(None, every, None),
            P(None, every, None),
            P(every),
            P(None, f, None),
            P(None, f, None),
            P(),
            P(None, every, None),
            P(None, every, None),
            P(None, every, None),
            P("tp", None),
        )
        out_specs = (P(f, "tp"), P())
        body = jax.shard_map(
            functools.partial(local, sizes), mesh=split, in_specs=in_specs, out_specs=out_specs,
            check_vma=False,
        )
        return body(*args)

    return run
```

```python
import functools
import math

import jax
import jax.numpy as jnp
from jax import lax
from jax.experimental import pallas as pl
from jax.experimental.pallas import tpu as pltpu
from jax.sharding import Mesh, PartitionSpec as P


QH = 64
KVH = 4
HD = 128
BLOCK = 128
WIN = 8

neg_fill = -1e30
epsilon = 1e-06
fp_limit = 448.0
f32 = jnp.float32
bf16 = jnp.bfloat16


def swap(value, axis, size, distance):
    return lax.ppermute(value, axis, [(i, i ^ distance) for i in range(size)])


def swaps(value, axis, size):
    return [value] + [swap(value, axis, size, s) for s in range(1, size)]


def attention_rows(queries, cache_keys, cache_values, fresh_keys, fresh_values, lengths):
    steps, row_count = queries.shape[:2]
    positions = cache_keys.shape[1]
    group = QH // KVH
    score_scale = HD ** (-0.5)
    query_heads = queries.reshape(steps, row_count, KVH, group, HD)
    query_heads = jnp.transpose(query_heads, (1, 2, 0, 3, 4))
    query_heads = query_heads.reshape(row_count, KVH, steps * group, HD)
    key_heads = cache_keys.reshape(row_count, positions, KVH, HD)
    value_heads = cache_values.reshape(row_count, positions, KVH, HD)
    fresh_key_heads = fresh_keys.reshape(steps, row_count, KVH, HD)
    fresh_value_heads = fresh_values.reshape(steps, row_count, KVH, HD)
    cached_scores = (
        jnp.einsum("rkgd,rpkd->rkgp", query_heads, key_heads, preferred_element_type=f32)
        * score_scale
    )
    fresh_scores = (
        jnp.einsum("rkgd,srkd->rkgs", query_heads, fresh_key_heads, preferred_element_type=f32)
        * score_scale
    )
    alive_mask = (jnp.arange(positions, dtype=jnp.int32)[None, :] < lengths[:, None])[
        :, None, None, :
    ]
    step_of = jnp.arange(steps * group, dtype=jnp.int32) // group
    seen_mask = (jnp.arange(steps, dtype=jnp.int32)[None, :] <= step_of[:, None])[None, None]
    peak_score = jnp.maximum(
        jnp.max(jnp.where(alive_mask, cached_scores, neg_fill), axis=-1),
        jnp.max(jnp.where(seen_mask, fresh_scores, neg_fill), axis=-1),
    )
    cached_weights = jnp.where(alive_mask, jnp.exp(cached_scores - peak_score[..., None]), 0.0)
    fresh_weights = jnp.where(seen_mask, jnp.exp(fresh_scores - peak_score[..., None]), 0.0)
    weight_sum = jnp.sum(cached_weights, axis=-1) + jnp.sum(fresh_weights, axis=-1)
    cached_probs = (cached_weights / weight_sum[..., None]).astype(bf16)
    fresh_probs = (fresh_weights / weight_sum[..., None]).astype(bf16)
    output = jnp.einsum("rkgp,rpkd->rkgd", cached_probs, value_heads, preferred_element_type=f32)
    output = output + jnp.einsum(
        "rkgs,srkd->rkgd", fresh_probs, fresh_value_heads, preferred_element_type=f32
    )
    output = output.astype(bf16).reshape(row_count, KVH, steps, group * HD)
    return jnp.transpose(output, (2, 0, 1, 3)).reshape(steps, row_count, QH * HD)


def maxima_kernel(cut_ref, gate_ref, up_ref, down_ref, out_ref, *, step):
    cut = cut_ref[0]
    rows, width = gate_ref.shape[1], gate_ref.shape[2]
    span = min(width, 512)
    for j, source in enumerate((gate_ref, up_ref, down_ref)):

        @pl.loop(0, width, step=span)
        def _(col):
            cols = pl.ds(pl.multiple_of(col, span), span)
            pair = [jnp.zeros((min(step, 8), span), f32)] * 2
            for start in range(0, rows, step):
                values = jnp.abs(source[0, pl.ds(start, step), cols])
                if step > 8:
                    values = jnp.max(values.reshape(step // 8, 8, span), axis=0)
                inside = start < cut
                pair[0] = jnp.maximum(pair[0], jnp.where(inside, values, 0.0))
                pair[1] = jnp.maximum(pair[1], jnp.where(inside, 0.0, values))
            for side in range(2):
                out_ref[j, 0, pl.ds(side, 1), cols] = jnp.max(pair[side], axis=0, keepdims=True)


def maxima(cut, masters):
    experts, rows, width = masters[0].shape
    spec = pl.BlockSpec((1, rows, width), lambda e: (e, 0, 0))
    count = 3 * experts * rows * width
    return pl.pallas_call(
        functools.partial(maxima_kernel, step=math.gcd(rows, BLOCK)),
        grid=(experts,),
        in_specs=[pl.BlockSpec(memory_space=pltpu.SMEM), spec, spec, spec],
        out_specs=pl.BlockSpec((3, 1, 2, width), lambda e: (0, e, 0, 0)),
        out_shape=jax.ShapeDtypeStruct((3, experts, 2, width), f32),
        cost_estimate=pl.CostEstimate(flops=4 * count, bytes_accessed=4 * count, transcendentals=0),
    )(cut, *masters)


def convert_kernel(cut_ref, gain_ref, gate_ref, up_ref, down_ref, scale_ref, *refs, step):
    outs, (inv_ref, back_ref) = refs[:3], refs[3:]
    cut = cut_ref[0]
    rows, width = gate_ref.shape[1], gate_ref.shape[2]
    span = min(width, 512)
    for j in range(3):
        inv_ref[j] = (1.0 / scale_ref[j, 0]) * (1.0 + 2.0**-22)
        back_ref[j] = scale_ref[j, 0] * gain_ref[...] if j < 2 else scale_ref[j, 0]
    for j, (source, target) in enumerate(zip((gate_ref, up_ref, down_ref), outs)):

        @pl.loop(0, width, step=span)
        def _(col):
            cols = pl.ds(pl.multiple_of(col, span), span)
            low = min(step, 8)
            sides = [
                [jnp.broadcast_to(ref[j, pl.ds(side, 1), cols], (low, span)) for side in range(2)]
                for ref in (inv_ref, back_ref)
            ]
            for start in range(0, rows, step):
                inside = start < cut
                inv, back = [jnp.where(inside, side[0], side[1])[None] for side in sides]
                values = source[0, pl.ds(start, step), cols].reshape(step // low, low, span) * inv
                spread = values * (2.0**20 + 1.0)
                normal = spread - (spread - values)
                small = (values + 24576.0) - 24576.0
                rounded = jnp.where(jnp.abs(values) < 2.0**-6, small, normal)
                restored = (rounded * back).reshape(step, span)
                target[0, pl.ds(start, step), cols] = restored.astype(bf16)


def convert(cut, gain, masters, scales):
    experts, rows, width = masters[0].shape
    spec = pl.BlockSpec((1, rows, width), lambda e: (e, 0, 0))
    factor = pl.BlockSpec((3, 1, 2, width), lambda e: (0, e, 0, 0))
    count = 3 * experts * rows * width
    return pl.pallas_call(
        functools.partial(convert_kernel, step=math.gcd(rows, BLOCK)),
        grid=(experts,),
        in_specs=[
            pl.BlockSpec(memory_space=pltpu.SMEM),
            pl.BlockSpec((1, width), lambda e: (0, 0)),
            spec,
            spec,
            spec,
            factor,
        ],
        out_specs=[spec] * 3,
        out_shape=[jax.ShapeDtypeStruct((experts, rows, width), bf16)] * 3,
        scratch_shapes=[pltpu.VMEM((3, 2, width), f32)] * 2,
        cost_estimate=pl.CostEstimate(
            flops=12 * count, bytes_accessed=6 * count, transcendentals=0
        ),
    )(cut, gain, *masters, scales)


def group_max(value, axes, size):
    if size & (size - 1):
        return lax.pmax(value, axes)
    bit = 1
    while bit < size:
        other = lax.ppermute(value, axes, [(i, i ^ bit) for i in range(size)])
        value = jnp.maximum(value, other)
        bit *= 2
    return value


def gate_shares(routes, route_weights):
    total = jnp.sum(route_weights, axis=2)
    matches = routes[:, :, None, :] == jnp.arange(WIN, dtype=jnp.int32)[None, None, :, None]
    picked = jnp.sum(jnp.where(matches, route_weights[:, :, None, :], 0.0), axis=3)
    return picked / total[..., None]


def product(left, right, dims):
    return lax.dot_general(left, right, (dims, ((), ())), preferred_element_type=f32)


def expert_kernel(line, tps, cores, last, experts, place_ref, *refs):
    lefts, refs = refs[:tps], refs[tps:]
    rights, refs = refs[:line], refs[line:]
    weights, refs = refs[: 3 * cores], refs[3 * cores :]
    outs, refs = refs[:tps], refs[tps:]
    others, (rows_ref, extra_ref, act_ref, gate_ref, up_ref, down_ref, sems) = refs[:line], refs[line:]
    hidden, width = weights[0].shape
    rows, half = lefts[0].shape[1:]
    copies = []
    for j, target in enumerate((gate_ref, up_ref, down_ref)):
        for c in range(cores):
            spot = pl.ds(c * hidden, hidden)
            copies.append(
                pltpu.make_async_copy(weights[3 * c + j], target.at[spot], sems.at[j * cores + c])
            )
    for copy in copies:
        copy.start()

    for z in range(line):
        for t in range(tps):
            spot = pl.ds((z * tps + t) * rows, rows)
            rows_ref[spot, :half] = lefts[t][z]
            rows_ref[spot, half:] = rights[z][t, :, : width - half]
            extra_ref[spot, :] = rights[z][t, :, width - half :]

    lanes = extra_ref.shape[1]
    entry = lax.broadcasted_iota(jnp.int32, (lanes, hidden), 0)
    owner = lax.broadcasted_iota(jnp.int32, (lanes, hidden), 1) // (hidden // experts)
    chosen = ((entry == owner) | (entry == owner + experts)).astype(f32).astype(bf16)
    factor = product(extra_ref[...], chosen, ((1,), (0,)))
    chunk = BLOCK if hidden % BLOCK == 0 else hidden
    entry = lax.broadcasted_iota(jnp.int32, (lanes, chunk), 0)
    alone = ((entry == 2 * experts) | (entry == 2 * experts + 1)).astype(f32).astype(bf16)
    inverse_rms = product(extra_ref[...], alone, ((1,), (0,)))

    for copy in copies[: 2 * cores]:
        copy.wait()
    total = cores * hidden
    for at in range(0, total, chunk):
        pair = jnp.concatenate([gate_ref[pl.ds(at, chunk), :], up_ref[pl.ds(at, chunk), :]])
        both = product(rows_ref[...], pair, ((1,), (1,)))
        gate, up = both[:, :chunk] * inverse_rms, both[:, chunk:]
        inside = at % hidden
        act = gate / (1.0 + jnp.exp(-gate)) * up * factor[:, inside : inside + chunk]
        act_ref[at // chunk] = act.astype(bf16)

    for copy in copies[2 * cores :]:
        copy.wait()
    act = jnp.concatenate([act_ref[i] for i in range(total // chunk)], axis=1)
    if last:
        place = place_ref[0]
        part = width // tps
        first = outs[0].shape[-1]
        for r in range(tps):
            cols = pl.ds(pl.multiple_of((place ^ r) * part, part), part)
            result = product(act, down_ref[:, cols], ((1,), (0,))).astype(bf16)
            for z in range(line):
                for t in range(tps):
                    start = (z * tps + t) * rows
                    outs[r][z, place ^ t] = result[start : start + rows, :first]
                    others[z][r, place ^ t] = result[start : start + rows, first:]
    else:
        first = outs[0].shape[-1]
        span = math.gcd(first, 512)
        for begin, end in ((0, first), (first, width)):

            @pl.loop(begin, end, step=span)
            def _(col):
                cols = pl.ds(pl.multiple_of(col, span), span)
                result = product(act, down_ref[:, cols], ((1,), (0,))).astype(bf16)
                spot = pl.ds(pl.multiple_of(col - begin, span), span)
                for z in range(line):
                    for t in range(tps):
                        start = (z * tps + t) * rows
                        target = outs[t].at[z] if begin == 0 else others[z].at[t]
                        target[:, spot] = result[start : start + rows]


def experts_of(place, experts, lefts, rights, shared, last):
    tps, line, cores = len(lefts), len(rights), len(shared)
    rows, half = lefts[0].shape[1:]
    hidden, width = shared[0][0].shape
    extra = rights[0].shape[2] - (width - half)
    count = line * tps * rows
    chunk = BLOCK if hidden % BLOCK == 0 else hidden
    vmem = pl.BlockSpec(memory_space=pltpu.VMEM)
    hbm = pl.BlockSpec(memory_space=pltpu.HBM)
    part = width // tps if last else width
    first = part * 7 // 8 // BLOCK * BLOCK
    middle = (tps, rows) if last else (rows,)
    shapes = [(line, *middle, first)] * tps + [(tps, *middle, part - first)] * line
    return pl.pallas_call(
        functools.partial(expert_kernel, line, tps, cores, last, experts),
        in_specs=[pl.BlockSpec(memory_space=pltpu.SMEM)]
        + [vmem] * (tps + line)
        + [hbm] * (3 * cores),
        out_specs=[vmem] * len(shapes),
        out_shape=[jax.ShapeDtypeStruct(shape, bf16) for shape in shapes],
        scratch_shapes=[
            pltpu.VMEM((count, width), bf16),
            pltpu.VMEM((count, extra), bf16),
            pltpu.VMEM((cores * hidden // chunk, count, chunk), bf16),
            pltpu.VMEM((cores * hidden, width), bf16),
            pltpu.VMEM((cores * hidden, width), bf16),
            pltpu.VMEM((cores * hidden, width), bf16),
            pltpu.SemaphoreType.DMA((3 * cores,)),
        ],
        cost_estimate=pl.CostEstimate(
            flops=6 * count * width * cores * hidden,
            bytes_accessed=6 * cores * hidden * width,
            transcendentals=count * cores * hidden,
        ),
    )(place, *lefts, *rights, *[m for matrices in shared for m in matrices])


def local(sizes, hidden_in, queries, key_cache, value_cache, new_keys, new_values, lengths,
          routes, route_weights, norm_gain, gate_master, up_master, down_master, out_proj):
    fa, fb, cores, tps = sizes
    far, group, line = ("fa", "fb"), ("fb", "core", "tp"), fa * fb
    experts, shard, width = gate_master.shape
    tp_pos = lax.axis_index("tp")
    group_pos = lax.axis_index(group)
    rows = queries.shape[1]
    tiles = width // BLOCK
    masters = (gate_master, up_master, down_master)

    base = group_pos * shard
    first = base // BLOCK
    cut = (first + 1) * BLOCK - base
    count = fb * cores * tps * shard // BLOCK
    cut = cut.astype(jnp.int32).reshape(1)
    sides = maxima(cut, masters)
    sides = jnp.max(sides.reshape(3, experts, 2, tiles, BLOCK), axis=4)
    places = jnp.arange(count, dtype=jnp.int32)[None, None, :, None]
    partial_max = jnp.where(
        places == first,
        sides[:, :, :1],
        jnp.where(places == first + 1, sides[:, :, 1:], 0.0),
    )
    partial_max, queries = lax.optimization_barrier((partial_max, queries))
    block_max = group_max(partial_max, group, fb * cores * tps)
    scales = (block_max + epsilon) / fp_limit

    steps = queries.shape[0]
    heads = attention_rows(queries, key_cache, value_cache, new_keys, new_values, lengths)
    part = out_proj.shape[0]
    pieces = [lax.dynamic_slice_in_dim(heads, (tp_pos ^ s) * part, part, 2) for s in range(tps)]
    pieces = [pieces[0]] + [swap(pieces[s], "tp", tps, s) for s in range(1, tps)]

    joined = jnp.concatenate([piece[None] for piece in pieces])
    total = product(joined.reshape(-1, part), out_proj, ((1,), (0,)))
    total = total.reshape(tps, steps, rows, width)

    padded = jnp.concatenate([scales, jnp.ones_like(scales[:, :, :1])], axis=2)
    own_scales = lax.dynamic_slice_in_dim(padded, first, 2, 2)
    spread_scales = swaps(scales, "fa", fa)
    own_scales, total, spread_scales = lax.optimization_barrier((own_scales, total, spread_scales))
    addends = total[0]
    for s in range(1, tps):
        addends = addends + swap(total[s].astype(bf16), "tp", tps, s).astype(f32)
    spread = jnp.repeat(own_scales, BLOCK, axis=3)
    own = list(convert(cut, norm_gain.reshape(1, width), masters, spread))
    addends, own[0] = lax.optimization_barrier((addends, own[0]))
    own = [matrix.reshape(experts * shard, width) for matrix in own]
    shared = [own]
    for s in range(1, cores):
        shared.append([swap(matrix, "core", cores, s) for matrix in own])

    shares = gate_shares(routes, route_weights)
    shares = lax.dynamic_slice_in_dim(shares, tp_pos * rows, rows, 1)
    order = tp_pos ^ jnp.arange(tps, dtype=jnp.int32)

    def beside(mixed, share):
        values = mixed.astype(f32)
        inverse = lax.rsqrt(jnp.mean(values * values, axis=1, keepdims=True) + epsilon)
        share = share * inverse
        parts = []
        for value in (share, inverse):
            high = lax.reduce_precision(value, 8, 7)
            parts += [high, value - high]
        parts = jnp.concatenate(parts, axis=1)
        return jnp.pad(parts, ((0, 0), (0, BLOCK - parts.shape[1]))).astype(bf16)

    half = width * 3 // 4 // BLOCK * BLOCK

    def everyone(mixed, share):
        left = jnp.stack(swaps(mixed[:, :half], far, line))
        right = jnp.concatenate([mixed[:, half:], beside(mixed, share)], axis=1)
        right = jnp.stack(swaps(right, "tp", tps))
        return swaps(left, "tp", tps), swaps(right, far, line)

    def summed(parts, axis):
        parts = list(parts)
        total = parts[0].astype(f32)
        for s in range(1, len(parts)):
            total = total + swap(parts[s].astype(bf16), axis, len(parts), s).astype(f32)
        return total

    def total_of(parts):
        left = summed(summed(parts[:tps], "tp"), far)
        right = summed(summed(parts[tps:], far), "tp")
        return jnp.concatenate([left, right], axis=-1)

    place = tp_pos.astype(jnp.int32).reshape(1)
    current = lax.dynamic_slice_in_dim(hidden_in, tp_pos * rows, rows, 0).astype(f32)
    for step in range(steps):
        last = step == steps - 1
        mixed = (current + addends[step]).astype(bf16)
        lefts, rights = everyone(mixed, shares[step])
        parts = list(experts_of(place, experts, lefts, rights, shared, last))
        moe = total_of(parts)
        if last:
            own_rows = jnp.concatenate([jnp.stack([left[0] for left in lefts]), rights[0][..., : width - half]], axis=2)
            part = width // tps
            mixed = lax.dynamic_slice_in_dim(own_rows, tp_pos * part, part, 2)[order]
        current = (mixed.astype(f32) + moe).astype(bf16).astype(f32)
    spread = jnp.stack(spread_scales)
    spread = spread[lax.axis_index("fa") ^ jnp.arange(fa, dtype=jnp.int32)]
    scale_log2 = jnp.log2(jnp.moveaxis(spread, 0, 2).reshape(3, experts, fa * count, tiles))
    hidden_out = current.astype(bf16).reshape(tps * rows, width // tps)
    return (hidden_out, scale_log2)


def solution(mesh):
    fsdp, tps = mesh.shape["fsdp"], mesh.shape["tp"]
    cores = 2 if fsdp % 2 == 0 else 1

    def run(*args):
        shard = args[10].shape[1] // (fsdp * tps)
        devices = math.lcm(shard, BLOCK) // shard
        fb = fsdp // cores
        if devices % (cores * tps) == 0 and fb % (devices // (cores * tps)) == 0:
            fb = devices // (cores * tps)
        fa = fsdp // (cores * fb)
        sizes = (fa, fb, cores, tps)
        split = Mesh(mesh.devices.reshape(sizes), ("fa", "fb", "core", "tp"))
        f = ("fa", "fb", "core")
        every = f + ("tp",)
        in_specs = (
            P(f, None),
            P(None, every, None),
            P(every, None, None),
            P(every, None, None),
            P(None, every, None),
            P(None, every, None),
            P(every),
            P(None, f, None),
            P(None, f, None),
            P(),
            P(None, every, None),
            P(None, every, None),
            P(None, every, None),
            P("tp", None),
        )
        out_specs = (P(f, "tp"), P())
        body = jax.shard_map(
            functools.partial(local, sizes), mesh=split, in_specs=in_specs, out_specs=out_specs,
            check_vma=False,
        )
        return body(*args)

    return run
```
